32 devices in a mesh: dp: 8 (over z, x), mp: 4 (over y, core).
Axes of the slice: x: 2, y: 2, z: 4, core: 2. Of those that a mesh axis runs over, the one named last changes fastest.
Arguments:
- grads: bfloat16 [8, 4, 4096, 256], P('dp', 'mp'), may hold values from -6 to 6
- master: float32 [4, 4096, 256], P('mp', 'dp'), may hold values from -6 to 6
- m_codes: bfloat16 [4, 4096, 256], P('mp', 'dp'), may hold values from -1 to 1
- m_scale: float32 [4, 4096], P('mp', 'dp'), may hold values from 0.005 to 0.05
- v_codes: bfloat16 [4, 4096, 256], P('mp', 'dp'), may hold values from 0.049804688 to 1
- v_scale: float32 [4, 4096], P('mp', 'dp'), may hold values from 0.001 to 0.01
Outputs:
- master_out: float32 [4, 4096, 256], P('mp', 'dp')
- m_codes_out: bfloat16 [4, 4096, 256], P('mp', 'dp')
- m_scale_out: float32 [4, 4096], P('mp', 'dp')
- v_codes_out: bfloat16 [4, 4096, 256], P('mp', 'dp')
- v_scale_out: float32 [4, 4096], P('mp', 'dp')
- weights: bfloat16 [4, 4096, 256], P('mp')
The draws below stay inside these ranges and needn't reach their ends.
All inputs are finite; a program needn't handle non-finite values. Where the reference program divides by a largest or mean magnitude, that divisor is 1e-20 or more.
Results may differ from the reference program's by a relative error of at most 0.024.
Values may be sent and summed in bfloat16 or wider, within the bound.
A program may use at most 128 MiB of HBM per device.

```python
import math
import jax
import jax.numpy as jnp
from jax import lax

BLOCK = 256
OWNB = 512
STEP = 8
MPB = 4096
LEVELS = 3
N_DP = 8
N_MP = 4


def raised(array, rng, source, target, shards_of, factor):
    def block_of(dim):
        return (jnp.arange(array.shape[dim]) // (array.shape[dim] // shards_of)).reshape((-1,) + (1,) * (array.ndim - 1 - dim))

    one_side = jax.random.permutation(rng, shards_of)[block_of(target)]
    other_side = (block_of(target) + shards_of // 2) % shards_of
    return jnp.where((block_of(source) == one_side) | (block_of(source) == other_side), factor * array, array)


def level_of(stream_key, dims, cuts, smallest, largest):
    factor_of = 1.0
    for position, shards_of in cuts:
        heights = jax.random.uniform(jax.random.fold_in(jax.random.fold_in(stream_key, 6), position), (shards_of,), jnp.float32, smallest / len(cuts), largest / len(cuts))
        factor_of = factor_of * jnp.repeat(jnp.exp(heights), dims[position] // shards_of).reshape((-1,) + (1,) * (len(dims) - 1 - position))
    return factor_of


def gaussian(rng, shape, scale, bound, shards=(), kind=jnp.bfloat16):
    result = jax.random.normal(rng, shape, jnp.float32) * scale
    if len(shards) > 0:
        result = level_of(rng, shape, shards, -0.22, 0.18) * result
    return jnp.clip(result, min=-bound, max=bound).astype(kind)


def gaussian_with(key, shape, width, most, shards, heavy, kind=jnp.bfloat16):
    array = width * jax.random.normal(key, shape, jnp.float32)
    if shards:
        array = array * level_of(key, shape, shards, -0.22, 0.18)
    return jnp.clip(raised(array, jax.random.fold_in(key, 3), *heavy), -most, most).astype(kind)


def setup_inputs(seed: int = 0) -> dict:
    arg_keys = jax.random.split(jax.random.key(seed), 7)
    grads = gaussian_with(arg_keys[0], (N_DP, N_MP, MPB, BLOCK), 1.0, 6.0, ((0, 8), (1, 4)), (0, 2, 8, 2.0))
    master = gaussian(arg_keys[1], (N_MP, MPB, BLOCK), 1.0, 6.0, ((0, 4), (1, 8)), jnp.float32)
    m_codes = jnp.clip(jax.random.uniform(arg_keys[2], (N_MP, MPB, BLOCK), jnp.float32, -1.0, 1.0) * level_of(arg_keys[2], (N_MP, MPB, BLOCK), ((0, 4), (1, 8)), -0.4, 0.0), -1.0, 1.0).astype(jnp.bfloat16)
    m_scale = jnp.clip(jnp.exp(math.log(0.05) - 2.3025851 * jax.random.uniform(arg_keys[3], (N_MP, MPB), jnp.float32) ** level_of(arg_keys[3], (N_MP, MPB), ((0, 4), (1, 8)), -0.2, 0.2)), 0.005, 0.05)
    v_codes = jnp.clip(0.049804688 + 0.9501953 * jax.random.uniform(arg_keys[4], (N_MP, MPB, BLOCK), jnp.float32) ** level_of(arg_keys[4], (N_MP, MPB, BLOCK), ((0, 4), (1, 8)), -0.2, 0.2), 0.049804688, 1.0).astype(jnp.bfloat16)
    v_scale = jnp.clip(jnp.exp(math.log(0.01) - 2.30258502 * jax.random.uniform(arg_keys[5], (N_MP, MPB), jnp.float32) ** level_of(arg_keys[5], (N_MP, MPB), ((0, 4), (1, 8)), -0.2, 0.2)), 0.001, 0.01)
    return dict(grads=grads, master=master, m_codes=m_codes, m_scale=m_scale, v_codes=v_codes, v_scale=v_scale)


def block_code(values):
    scale = (lax.optimization_barrier(jnp.max(jnp.abs(values), axis=-1)) + 1e-06).astype(jnp.bfloat16)
    levels = (values / scale.astype(jnp.float32)[..., None]).astype(jnp.bfloat16)
    return (levels, scale)

def expand(levels, scale):
    return levels.astype(jnp.float32) * scale.astype(jnp.float32)[..., None]

def state_code(values):
    scale = lax.optimization_barrier(jnp.max(jnp.abs(values), axis=-1)) + 1e-06
    return ((values / scale[..., None]).astype(jnp.bfloat16), scale)

def pair_tree(values):
    for level in range(LEVELS - 1):
        pairs = values.reshape((values.shape[0] // 2, 2) + values.shape[1:])
        levels, scale = block_code(pairs[:, 0] + pairs[:, 1])
        values = expand(levels, scale)
    return values[0] + values[1]

def reference(grads, master, m_codes, m_scale, v_codes, v_scale):

    def owner_mean(index):
        shard = (index // N_DP).astype(jnp.int32)
        owner = (index % N_DP).astype(jnp.int32)
        zero = jnp.zeros((), jnp.int32)
        start = (owner * OWNB).astype(jnp.int32)
        piece = lax.dynamic_slice(grads, (zero, shard, start, zero), (N_DP, 1, OWNB, BLOCK))[:, 0]
        levels, scale = block_code(piece.astype(jnp.float32))
        return pair_tree(expand(levels, scale)) / N_DP
    indices = jnp.arange(N_MP * N_DP, dtype=jnp.int32)
    grad_mean = lax.map(owner_mean, indices).reshape(N_MP, MPB, BLOCK)
    moment_one = 0.9 * m_codes.astype(jnp.float32) * m_scale[..., None] + 0.1 * grad_mean
    moment_two = 0.95 * v_codes.astype(jnp.float32) * v_scale[..., None] + 0.05 * grad_mean * grad_mean
    first_fix = 1.0 - 0.9 ** STEP
    second_fix = 1.0 - 0.95 ** STEP
    master_out = master - 0.1 * (moment_one / first_fix) / (jnp.sqrt(moment_two / second_fix) + 1e-08)
    one_code, one_scale = state_code(moment_one)
    two_code, two_scale = state_code(moment_two)
    weights = master_out.astype(jnp.bfloat16)
    return (master_out, one_code, one_scale, two_code, two_scale, weights)
```

```python
import functools

import jax
import jax.numpy as jnp
from jax import lax
from jax.experimental import pallas as pl
from jax.experimental.pallas import tpu as pltpu
from jax.sharding import PartitionSpec as P

STEP = 8
ROWS = 128
MESH = pl.DeviceIdType.MESH


def spread(row):
    return jnp.transpose(jnp.broadcast_to(row, (ROWS, ROWS)))


def gather_row(column):
    return jnp.transpose(jnp.broadcast_to(column, (ROWS, ROWS)))[0:1, :]


def kernel(
    outer, grads, master, m_codes, m_scale, v_codes, v_scale,
    master_out, m_out, ms_out, v_out, vs_out, weights,
    own, xgot, stage, mine, zgot, wbuf,
    master_in, m_in, v_in, ms_in, vs_in, master_new, m_new, v_new, ms_new, vs_new,
    own_sem, state_sem, out_sem, wout_sem,
    xs_send, xs_recv, zs_send, zs_recv, zg_send, zg_recv, xg_send, xg_recv,
):
    owned, width = master.shape[1], master.shape[2]
    pieces = owned // ROWS
    replicas = 2 * outer
    me = lax.axis_index("dp")
    x = lax.rem(me, 2)
    z = lax.div(me, 2)
    other = z * 2 + 1 - x

    def ahead(step):
        return lax.rem(z + 1 + step, outer)

    def behind(step):
        return lax.rem(z + 2 * outer - 1 - step, outer)

    def rows_of(owner, piece):
        return pl.ds(pl.multiple_of(owner * owned + piece * ROWS, ROWS), ROWS)

    def remote(src, dst, send, recv, device):
        return pltpu.make_async_remote_copy(
            src_ref=src, dst_ref=dst, send_sem=send, recv_sem=recv,
            device_id={"dp": device}, device_id_type=MESH,
        )

    barrier = pltpu.get_barrier_semaphore()
    pl.semaphore_signal(barrier, inc=1, device_id={"dp": other}, device_id_type=MESH)
    for step in range(outer - 1):
        pl.semaphore_signal(
            barrier, inc=1, device_id={"dp": ahead(step) * 2 + x}, device_id_type=MESH
        )

    own_copies = {}
    for k in range(pieces):
        for step in range(outer):
            copy = pltpu.make_async_copy(
                grads.at[0, 0, rows_of(ahead(step) * 2 + x, k), :],
                own.at[k, step], own_sem.at[k, step],
            )
            copy.start()
            own_copies[k, step] = copy
    state_copies = []
    for i, (src, dst) in enumerate((
        (master, master_in), (m_codes, m_in), (v_codes, v_in), (m_scale, ms_in), (v_scale, vs_in),
    )):
        copy = pltpu.make_async_copy(src, dst, state_sem.at[i])
        copy.start()
        state_copies.append(copy)

    pl.semaphore_wait(barrier, outer)
    xs = {}
    for k in range(pieces):
        for step in range(outer):
            copy = remote(
                grads.at[0, 0, rows_of(ahead(step) * 2 + 1 - x, k), :], xgot.at[k, step],
                xs_send.at[k, step], xs_recv.at[k, step], other,
            )
            copy.start()
            xs[k, step] = copy

    zs, zg, xg, locals_ = {}, {}, {}, []

    def pair_sums(k):
        for step in range(outer):
            own_copies[k, step].wait()
            xs[k, step].wait_recv()
            total = own[k, step].astype(jnp.float32) + xgot[k, step].astype(jnp.float32)
            if step == outer - 1:
                mine[k] = total
            else:
                stage[k, step] = total.astype(jnp.bfloat16)
                copy = remote(
                    stage.at[k, step], zgot.at[k, step],
                    zs_send.at[k, step], zs_recv.at[k, step], ahead(step) * 2 + x,
                )
                copy.start()
                zs[k, step] = copy

    def update(k):
        if k == 0:
            for copy in state_copies:
                copy.wait()
        rows = pl.ds(k * ROWS, ROWS)
        total = mine[k]
        for step in range(outer - 1):
            zs[k, step].wait_recv()
            total = total + zgot[k, step].astype(jnp.float32)
        mean = total * (1.0 / replicas)
        ms = spread(ms_in[0:1, rows])
        vs = spread(vs_in[0:1, rows])
        ms = jnp.concatenate([ms] * (width // ROWS), axis=1)
        vs = jnp.concatenate([vs] * (width // ROWS), axis=1)
        one = 0.9 * m_in[0, rows].astype(jnp.float32) * ms + 0.1 * mean
        two = 0.95 * v_in[0, rows].astype(jnp.float32) * vs + 0.05 * mean * mean
        first_fix = 1.0 - 0.9**STEP
        second_fix = 1.0 - 0.95**STEP
        new = master_in[0, rows] - (0.1 / first_fix) * one / (
            jnp.sqrt(two * (1.0 / second_fix)) + 1e-08
        )
        wbuf[z, rows] = new.astype(jnp.bfloat16)
        for step in range(outer - 1):
            copy = remote(
                wbuf.at[z, rows], wbuf.at[z, rows],
                zg_send.at[k, step], zg_recv.at[k, step], ahead(step) * 2 + x,
            )
            copy.start()
            zg[k, step] = copy
        pass_on(k, outer - 1, z)
        master_new[0, rows] = new
        one_top = jnp.max(jnp.abs(one), axis=-1, keepdims=True) + 1e-06
        two_top = jnp.max(jnp.abs(two), axis=-1, keepdims=True) + 1e-06
        m_new[0, rows] = (one / one_top).astype(jnp.bfloat16)
        v_new[0, rows] = (two / two_top).astype(jnp.bfloat16)
        ms_new[0:1, rows] = gather_row(one_top)
        vs_new[0:1, rows] = gather_row(two_top)
        for i, (src, dst) in enumerate((
            (master_new, master_out), (m_new, m_out), (v_new, v_out),
        )):
            copy = pltpu.make_async_copy(src.at[0, rows], dst.at[0, rows], out_sem.at[k, i])
            copy.start()
            locals_.append(copy)

    def pass_on(k, step, source):
        rows = pl.ds(k * ROWS, ROWS)
        target = weights.at[0, rows_of(source * 2 + x, k), :]
        copy = remote(
            wbuf.at[source, rows], target, xg_send.at[k, step], xg_recv.at[k, step], other
        )
        copy.start()
        xg[k, step] = copy
        local = pltpu.make_async_copy(wbuf.at[source, rows], target, wout_sem.at[k, step])
        local.start()
        locals_.append(local)

    def forward(k):
        for step in range(outer - 1):
            zg[k, step].wait_recv()
            pass_on(k, step, behind(step))

    for tick in range(pieces + 2):
        if tick < pieces:
            pair_sums(tick)
        if 0 <= tick - 1 < pieces:
            update(tick - 1)
            if tick == pieces:
                for i, (src, dst) in enumerate(((ms_new, ms_out), (vs_new, vs_out))):
                    copy = pltpu.make_async_copy(src, dst, state_sem.at[i])
                    copy.start()
                    locals_.append(copy)
        if 0 <= tick - 2 < pieces:
            forward(tick - 2)

    for group in (xs, zs, zg, xg):
        for copy in group.values():
            copy.wait_send()
    for copy in xg.values():
        copy.wait_recv()
    for copy in locals_:
        copy.wait()


def per_device(grads, master, m_codes, m_scale, v_codes, v_scale):
    outer = lax.axis_size("dp") // 2
    _, owned, width = master.shape
    pieces = owned // ROWS
    bf16, f32 = jnp.bfloat16, jnp.float32
    dma = pltpu.SemaphoreType.DMA
    shape = jax.ShapeDtypeStruct
    state = (1, owned, width)
    outs = pl.pallas_call(
        functools.partial(kernel, outer),
        out_shape=(
            shape(state, f32), shape(state, bf16), shape((1, owned), f32),
            shape(state, bf16), shape((1, owned), f32),
            shape((1, 2 * outer * owned, width), bf16),
        ),
        in_specs=[pl.BlockSpec(memory_space=pl.ANY)] * 6,
        out_specs=[pl.BlockSpec(memory_space=pl.ANY)] * 6,
        scratch_shapes=[
            pltpu.VMEM((pieces, outer, ROWS, width), bf16),
            pltpu.VMEM((pieces, outer, ROWS, width), bf16),
            pltpu.VMEM((pieces, outer - 1, ROWS, width), bf16),
            pltpu.VMEM((pieces, ROWS, width), f32),
            pltpu.VMEM((pieces, outer - 1, ROWS, width), bf16),
            pltpu.VMEM((outer, owned, width), bf16),
            pltpu.VMEM(state, f32), pltpu.VMEM(state, bf16), pltpu.VMEM(state, bf16),
            pltpu.VMEM((1, owned), f32), pltpu.VMEM((1, owned), f32),
            pltpu.VMEM(state, f32), pltpu.VMEM(state, bf16), pltpu.VMEM(state, bf16),
            pltpu.VMEM((1, owned), f32), pltpu.VMEM((1, owned), f32),
            dma((pieces, outer)), dma((5,)), dma((pieces, 3)), dma((pieces, outer)),
            dma((pieces, outer)), dma((pieces, outer)),
            dma((pieces, outer - 1)), dma((pieces, outer - 1)),
            dma((pieces, outer - 1)), dma((pieces, outer - 1)),
            dma((pieces, outer)), dma((pieces, outer)),
        ],
        compiler_params=pltpu.CompilerParams(collective_id=0, has_side_effects=True),
    )(grads, master, m_codes, m_scale, v_codes, v_scale)
    return tuple(outs)


def solution(mesh):
    return jax.shard_map(
        per_device,
        mesh=mesh,
        in_specs=(
            P("dp", "mp", None, None),
            P("mp", "dp", None),
            P("mp", "dp", None),
            P("mp", "dp"),
            P("mp", "dp", None),
            P("mp", "dp"),
        ),
        out_specs=(
            P("mp", "dp", None),
            P("mp", "dp", None),
            P("mp", "dp"),
            P("mp", "dp", None),
            P("mp", "dp"),
            P("mp", None, None),
        ),
        check_vma=False,
    )
```

```python
import functools
import math

import jax
import jax.numpy as jnp
from jax import lax
from jax.experimental import pallas as pl
from jax.experimental.pallas import tpu as pltpu
from jax.sharding import PartitionSpec as P

STEP = 8
ROWS = 128
VMEM_ALL = 67043328
VMEM_GRANT = 60 * 1024 * 1024
MESH = pl.DeviceIdType.MESH


def spread(row):
    return jnp.transpose(jnp.broadcast_to(row, (ROWS, ROWS)))


def gather_row(column):
    return jnp.transpose(jnp.broadcast_to(column, (ROWS, ROWS)))[0:1, :]


def kernel(
    outer, grads, master, m_codes, m_scale, v_codes, v_scale,
    master_new, m_new, ms_new, v_new, vs_new, weights,
    own, xgot, stage, mine, zgot,
    master_in, m_in, v_in, ms_in, vs_in,
    own_sem, state_sem,
    xs_send, xs_recv, zs_send, zs_recv, right_send, left_send, zg_recv, xg_send, xg_recv,
):
    owned, width = master.shape[1], master.shape[2]
    pieces = owned // ROWS
    replicas = 2 * outer
    me = lax.axis_index("dp")
    x = lax.rem(me, 2)
    z = lax.div(me, 2)
    other = z * 2 + 1 - x

    def ahead(step):
        return lax.rem(z + 1 + step, outer)

    def rows_of(owner, piece):
        return pl.ds(pl.multiple_of(owner * owned + piece * ROWS, ROWS), ROWS)

    def remote(src, dst, send, recv, device):
        return pltpu.make_async_remote_copy(
            src_ref=src, dst_ref=dst, send_sem=send, recv_sem=recv,
            device_id={"dp": device}, device_id_type=MESH,
        )

    barrier = pltpu.get_barrier_semaphore()
    pl.semaphore_signal(barrier, inc=1, device_id={"dp": other}, device_id_type=MESH)
    for step in range(outer - 1):
        pl.semaphore_signal(
            barrier, inc=1, device_id={"dp": ahead(step) * 2 + x}, device_id_type=MESH
        )

    own_copies = {}
    for k in range(pieces):
        for step in range(outer):
            copy = pltpu.make_async_copy(
                grads.at[0, 0, rows_of(ahead(step) * 2 + x, k), :],
                own.at[k, step], own_sem.at[k, step],
            )
            copy.start()
            own_copies[k, step] = copy
    state_copies = []
    for i, (src, dst) in enumerate((
        (master, master_in), (m_codes, m_in), (v_codes, v_in), (m_scale, ms_in), (v_scale, vs_in),
    )):
        copy = pltpu.make_async_copy(src, dst, state_sem.at[i])
        copy.start()
        state_copies.append(copy)

    pl.semaphore_wait(barrier, outer)
    xs = {}
    for k in range(pieces):
        for step in range(outer):
            copy = remote(
                grads.at[0, 0, rows_of(ahead(step) * 2 + 1 - x, k), :], xgot.at[k, step],
                xs_send.at[k, step], xs_recv.at[k, step], other,
            )
            copy.start()
            xs[k, step] = copy

    zs = {}

    def pair_sums(k):
        for step in range(outer):
            own_copies[k, step].wait()
            xs[k, step].wait_recv()
            total = own[k, step].astype(jnp.float32) + xgot[k, step].astype(jnp.float32)
            if step == outer - 1:
                mine[k] = total
            else:
                stage[k, step] = total.astype(jnp.bfloat16)
                copy = remote(
                    stage.at[k, step], zgot.at[k, step],
                    zs_send.at[k, step], zs_recv.at[k, step], ahead(step) * 2 + x,
                )
                copy.start()
                zs[k, step] = copy

    def weight_rows(k, source):
        return weights.at[0, rows_of(source * 2 + x, k), :]

    def rightward(k, source):
        rows = weight_rows(k, source)
        return remote(
            rows, rows, right_send.at[k, source], zg_recv.at[k, source],
            lax.min(z + 1, outer - 1) * 2 + x,
        )

    def leftward(k, source):
        rows = weight_rows(k, source)
        return remote(
            rows, rows, left_send.at[k, source], zg_recv.at[k, source],
            lax.max(z - 1, 0) * 2 + x,
        )

    def across(k, source):
        rows = weight_rows(k, source)
        return remote(rows, rows, xg_send.at[k, source], xg_recv.at[k, source], other)

    def update(k):
        if k == 0:
            for copy in state_copies:
                copy.wait()
        rows = pl.ds(k * ROWS, ROWS)
        total = mine[k]
        for step in range(outer - 1):
            zs[k, step].wait_recv()
            total = total + zgot[k, step].astype(jnp.float32)
        mean = total * (1.0 / replicas)
        ms = spread(ms_in[0:1, rows])
        vs = spread(vs_in[0:1, rows])
        ms = jnp.concatenate([ms] * (width // ROWS), axis=1)
        vs = jnp.concatenate([vs] * (width // ROWS), axis=1)
        one = 0.9 * m_in[0, rows].astype(jnp.float32) * ms + 0.1 * mean
        two = 0.95 * v_in[0, rows].astype(jnp.float32) * vs + 0.05 * mean * mean
        first_fix = 1.0 - 0.9**STEP
        second_fix = 1.0 - 0.95**STEP
        new = master_in[0, rows] - (0.1 / first_fix) * one / (
            jnp.sqrt(two * (1.0 / second_fix)) + 1e-08
        )
        weights[0, rows_of(me, k), :] = new.astype(jnp.bfloat16)
        pl.when(z < outer - 1)(lambda: rightward(k, z).start())
        pl.when(z > 0)(lambda: leftward(k, z).start())
        across(k, z).start()
        master_new[0, rows] = new
        one_top = jnp.max(jnp.abs(one), axis=-1, keepdims=True) + 1e-06
        two_top = jnp.max(jnp.abs(two), axis=-1, keepdims=True) + 1e-06
        m_new[0, rows] = (one / one_top).astype(jnp.bfloat16)
        v_new[0, rows] = (two / two_top).astype(jnp.bfloat16)
        ms_new[0:1, rows] = gather_row(one_top)
        vs_new[0:1, rows] = gather_row(two_top)

    def forward(k, apart):
        @pl.when(z >= apart)
        def _():
            source = z - apart
            rightward(k, source).wait_recv()
            pl.when(z < outer - 1)(lambda: rightward(k, source).start())
            across(k, source).start()

        @pl.when(z + apart < outer)
        def _():
            source = z + apart
            leftward(k, source).wait_recv()
            pl.when(z > 0)(lambda: leftward(k, source).start())
            across(k, source).start()

    for tick in range(pieces + outer):
        if tick < pieces:
            pair_sums(tick)
        if 0 <= tick - 1 < pieces:
            update(tick - 1)
        for apart in range(1, outer):
            if 0 <= tick - 1 - apart < pieces:
                forward(tick - 1 - apart, apart)

    for group in (xs, zs):
        for copy in group.values():
            copy.wait_send()
    for k in range(pieces):
        for source in range(outer):
            across(k, source).wait_send()
            pl.when((source <= z) & (z < outer - 1))(lambda: rightward(k, source).wait_send())
            pl.when((source >= z) & (z > 0))(lambda: leftward(k, source).wait_send())
    for k in range(pieces):
        for source in range(outer):
            across(k, source).wait_recv()


def write_out(*refs):
    sem = refs[-1]
    half = (len(refs) - 1) // 2
    copies = [
        pltpu.make_async_copy(refs[i], refs[half + i], sem.at[i]) for i in range(half)
    ]
    for copy in copies[::-1]:
        copy.start()
    for copy in copies:
        copy.wait()


def per_device(grads, master, m_codes, m_scale, v_codes, v_scale):
    outer = lax.axis_size("dp") // 2
    _, owned, width = master.shape
    pieces = owned // ROWS
    bf16, f32 = jnp.bfloat16, jnp.float32
    dma = pltpu.SemaphoreType.DMA
    shape = jax.ShapeDtypeStruct
    state = (1, owned, width)
    out_shapes = (
        (state, f32), (state, bf16), ((1, owned), f32),
        (state, bf16), ((1, owned), f32),
        ((1, 2 * outer * owned, width), bf16),
    )
    kept = sum(math.prod(dims) * jnp.dtype(kind).itemsize for dims, kind in out_shapes)
    outs = pl.pallas_call(
        functools.partial(kernel, outer),
        out_shape=tuple(pltpu.VMEM(*each) for each in out_shapes),
        in_specs=[pl.BlockSpec(memory_space=pltpu.HBM)] * 6,
        out_specs=[pl.BlockSpec(memory_space=pltpu.VMEM)] * 6,
        scratch_shapes=[
            pltpu.VMEM((pieces, outer, ROWS, width), bf16),
            pltpu.VMEM((pieces, outer, ROWS, width), bf16),
            pltpu.VMEM((pieces, outer - 1, ROWS, width), bf16),
            pltpu.VMEM((pieces, ROWS, width), f32),
            pltpu.VMEM((pieces, outer - 1, ROWS, width), bf16),
            pltpu.VMEM(state, f32), pltpu.VMEM(state, bf16), pltpu.VMEM(state, bf16),
            pltpu.VMEM((1, owned), f32), pltpu.VMEM((1, owned), f32),
            dma((pieces, outer)), dma((5,)),
            dma((pieces, outer)), dma((pieces, outer)),
            dma((pieces, outer - 1)), dma((pieces, outer - 1)),
            dma((pieces, outer)), dma((pieces, outer)), dma((pieces, outer)),
            dma((pieces, outer)), dma((pieces, outer)),
        ],
        compiler_params=pltpu.CompilerParams(
            collective_id=0, has_side_effects=True,
            vmem_limit_bytes=min(VMEM_GRANT, VMEM_ALL - kept - 2**18),
        ),
    )(grads, master, m_codes, m_scale, v_codes, v_scale)
    return tuple(pl.pallas_call(
        write_out,
        out_shape=tuple(shape(*each) for each in out_shapes),
        in_specs=[pl.BlockSpec(memory_space=pltpu.VMEM)] * 6,
        out_specs=[pl.BlockSpec(memory_space=pl.ANY)] * 6,
        scratch_shapes=[dma((6,))],
        compiler_params=pltpu.CompilerParams(vmem_limit_bytes=2**20),
    )(*[pltpu.with_memory_space_constraint(o, pltpu.VMEM) for o in outs]))


def solution(mesh):
    return jax.shard_map(
        per_device,
        mesh=mesh,
        in_specs=(
            P("dp", "mp", None, None),
            P("mp", "dp", None),
            P("mp", "dp", None),
            P("mp", "dp"),
            P("mp", "dp", None),
            P("mp", "dp"),
        ),
        out_specs=(
            P("mp", "dp", None),
            P("mp", "dp", None),
            P("mp", "dp"),
            P("mp", "dp", None),
            P("mp", "dp"),
            P("mp", None, None),
        ),
        check_vma=False,
    )
```

```python
import functools
import math

import jax
import jax.numpy as jnp
from jax import lax
from jax.experimental import pallas as pl
from jax.experimental.pallas import tpu as pltpu
from jax.sharding import PartitionSpec as P

STEP = 8
ROWS = 128
VMEM_ALL = 67043328
VMEM_GRANT = 60 * 1024 * 1024
MESH = pl.DeviceIdType.MESH


def spread(row):
    return jnp.transpose(jnp.broadcast_to(row, (ROWS, ROWS)))


def gather_row(column):
    return jnp.transpose(jnp.broadcast_to(column, (ROWS, ROWS)))[0:1, :]


def kernel(
    outer, grads, master, m_codes, m_scale, v_codes, v_scale,
    master_new, m_new, ms_new, v_new, vs_new, weights,
    own, xgot, stage, mine, pgot, zgot,
    master_in, m_in, v_in, ms_in, vs_in,
    own_sem, state_sem,
    xs_send, xs_recv, zs_send, pair_recv, zs_recv,
    right_send, left_send, zg_recv, xg_send, xg_recv,
):
    owned, width = master.shape[1], master.shape[2]
    pieces = owned // ROWS
    replicas = 2 * outer
    me = lax.axis_index("dp")
    x = lax.rem(me, 2)
    z = lax.div(me, 2)
    other = z * 2 + 1 - x
    odd = lax.rem(z, 2)
    pair = z + 1 - 2 * odd
    given = z * odd + (outer - 1 - z) * (1 - odd)
    x_first = pieces // 2

    def target(step):
        return step * odd + (outer - 1 - step) * (1 - odd)

    def ahead(step):
        return lax.rem(z + 1 + step, outer)

    def rows_of(owner, piece):
        return pl.ds(pl.multiple_of(owner * owned + piece * ROWS, ROWS), ROWS)

    def remote(src, dst, send, recv, device):
        return pltpu.make_async_remote_copy(
            src_ref=src, dst_ref=dst, send_sem=send, recv_sem=recv,
            device_id={"dp": device}, device_id_type=MESH,
        )

    barrier = pltpu.get_barrier_semaphore()
    pl.semaphore_signal(barrier, inc=1, device_id={"dp": other}, device_id_type=MESH)
    for step in range(outer - 1):
        pl.semaphore_signal(
            barrier, inc=1, device_id={"dp": ahead(step) * 2 + x}, device_id_type=MESH
        )

    own_copies = {}
    for k in range(pieces):
        for step in range(outer):
            copy = pltpu.make_async_copy(
                grads.at[0, 0, rows_of(target(step) * 2 + x, k), :],
                own.at[k, step], own_sem.at[k, step],
            )
            copy.start()
            own_copies[k, step] = copy
    state_copies = []
    for i, (src, dst) in enumerate((
        (master, master_in), (m_codes, m_in), (v_codes, v_in), (m_scale, ms_in), (v_scale, vs_in),
    )):
        copy = pltpu.make_async_copy(src, dst, state_sem.at[i])
        copy.start()
        state_copies.append(copy)

    pl.semaphore_wait(barrier, outer)
    xs = {}

    def send_pairs(k):
        for step in range(outer):
            copy = remote(
                grads.at[0, 0, rows_of(target(step) * 2 + 1 - x, k), :], xgot.at[k, step],
                xs_send.at[k, step], xs_recv.at[k, step], other,
            )
            copy.start()
            xs[k, step] = copy

    def to_pair(k, step):
        return remote(
            stage.at[k, step], pgot.at[k, target(step)],
            zs_send.at[k, step], pair_recv.at[k, target(step)], pair * 2 + x,
        )

    def to_owner(k, step, slot):
        return remote(
            stage.at[k, step], zgot.at[k, slot],
            zs_send.at[k, step], zs_recv.at[k, slot], target(step) * 2 + x,
        )

    def pair_sum(k, step):
        return own[k, step].astype(jnp.float32) + xgot[k, step].astype(jnp.float32)

    def pair_sums(k):
        for step in range(outer):
            own_copies[k, step].wait()
            xs[k, step].wait_recv()

            @pl.when(step < given)
            def _():
                stage[k, step] = pair_sum(k, step).astype(jnp.bfloat16)
                to_pair(k, step).start()

            @pl.when(step == given)
            def _():
                mine[k] = pair_sum(k, step)

    def merges(k):
        for step in range(1, outer):

            @pl.when(step > given)
            def _():
                to_pair(k, step).wait_recv()
                total = pair_sum(k, step) + pgot[k, target(step)].astype(jnp.float32)
                stage[k, step] = total.astype(jnp.bfloat16)
                to_owner(k, step, lax.div(z, 2)).start()

    def weight_rows(k, chunk):
        return weights.at[0, rows_of(chunk, k), :]

    def rightward(k, chunk):
        rows = weight_rows(k, chunk)
        return remote(
            rows, rows, right_send.at[k, chunk], zg_recv.at[k, chunk],
            lax.min(z + 1, outer - 1) * 2 + x,
        )

    def leftward(k, chunk):
        rows = weight_rows(k, chunk)
        return remote(
            rows, rows, left_send.at[k, chunk], zg_recv.at[k, chunk],
            lax.max(z - 1, 0) * 2 + x,
        )

    def across(k, source):
        rows = weight_rows(k, source * 2 + x)
        return remote(rows, rows, xg_send.at[k, source], xg_recv.at[k, source], other)

    def both_ways(k, chunk):
        pl.when(z < outer - 1)(lambda: rightward(k, chunk).start())
        pl.when(z > 0)(lambda: leftward(k, chunk).start())

    def update(k):
        if k == 0:
            for copy in state_copies:
                copy.wait()
        rows = pl.ds(k * ROWS, ROWS)
        total = mine[k]
        remote(
            stage.at[k, 0], pgot.at[k, z], zs_send.at[k, 0], pair_recv.at[k, z], pair * 2 + x
        ).wait_recv()
        total = total + pgot[k, z].astype(jnp.float32)
        for i in range(outer // 2 - 1):
            slot = lax.rem(lax.div(z, 2) + 1 + i, outer // 2)
            to_owner(k, 0, slot).wait_recv()
            total = total + zgot[k, slot].astype(jnp.float32)
        mean = total * (1.0 / replicas)
        ms = spread(ms_in[0:1, rows])
        vs = spread(vs_in[0:1, rows])
        ms = jnp.concatenate([ms] * (width // ROWS), axis=1)
        vs = jnp.concatenate([vs] * (width // ROWS), axis=1)
        one = 0.9 * m_in[0, rows].astype(jnp.float32) * ms + 0.1 * mean
        two = 0.95 * v_in[0, rows].astype(jnp.float32) * vs + 0.05 * mean * mean
        first_fix = 1.0 - 0.9**STEP
        second_fix = 1.0 - 0.95**STEP
        new = master_in[0, rows] - (0.1 / first_fix) * one / (
            jnp.sqrt(two * (1.0 / second_fix)) + 1e-08
        )
        weights[0, rows_of(me, k), :] = new.astype(jnp.bfloat16)
        if k < x_first:
            across(k, z).start()
            both_ways(k, me)
        else:
            both_ways(k, me)
            across(k, z).start()
        master_new[0, rows] = new
        one_top = jnp.max(jnp.abs(one), axis=-1, keepdims=True) + 1e-06
        two_top = jnp.max(jnp.abs(two), axis=-1, keepdims=True) + 1e-06
        m_new[0, rows] = (one / one_top).astype(jnp.bfloat16)
        v_new[0, rows] = (two / two_top).astype(jnp.bfloat16)
        ms_new[0:1, rows] = gather_row(one_top)
        vs_new[0:1, rows] = gather_row(two_top)

    def from_partner(k):
        across(k, z).wait_recv()
        both_ways(k, other)

    def forward(k, apart, side):
        @pl.when(z >= apart)
        def _():
            chunk = (z - apart) * 2 + side
            rightward(k, chunk).wait_recv()
            pl.when(z < outer - 1)(lambda: rightward(k, chunk).start())
            if k >= x_first:
                across(k, z - apart).start()

        @pl.when(z + apart < outer)
        def _():
            chunk = (z + apart) * 2 + side
            leftward(k, chunk).wait_recv()
            pl.when(z > 0)(lambda: leftward(k, chunk).start())
            if k >= x_first:
                across(k, z + apart).start()

    for k in range(min(2, pieces)):
        send_pairs(k)
    for tick in range(pieces + outer + 2):
        if tick < pieces:
            pair_sums(tick)
        if 0 <= tick - 1 < pieces:
            update(tick - 1)
        if tick + 2 < pieces:
            send_pairs(tick + 2)
        if tick < pieces:
            merges(tick)
        if 0 <= tick - 3 < x_first:
            from_partner(tick - 3)
        for apart in range(1, outer):
            if 0 <= tick - 1 - apart < pieces:
                forward(tick - 1 - apart, apart, x)
            if 0 <= tick - 3 - apart < x_first:
                forward(tick - 3 - apart, apart, 1 - x)

    for copy in xs.values():
        copy.wait_send()
    for k in range(pieces):
        for step in range(outer):
            pl.when(step != given)(lambda: to_pair(k, step).wait_send())
        for source in range(outer):
            for side in (x, 1 - x) if k < x_first else (x,):
                chunk = source * 2 + side
                pl.when((source <= z) & (z < outer - 1))(lambda: rightward(k, chunk).wait_send())
                pl.when((source >= z) & (z > 0))(lambda: leftward(k, chunk).wait_send())
        for source in (z,) if k < x_first else range(outer):
            across(k, source).wait_send()
    for k in range(x_first, pieces):
        for source in range(outer):
            across(k, source).wait_recv()


def write_out(*refs):
    sem = refs[-1]
    half = (len(refs) - 1) // 2
    copies = [
        pltpu.make_async_copy(refs[i], refs[half + i], sem.at[i]) for i in range(half)
    ]
    for copy in copies[::-1]:
        copy.start()
    for copy in copies:
        copy.wait()


def per_device(grads, master, m_codes, m_scale, v_codes, v_scale):
    outer = lax.axis_size("dp") // 2
    _, owned, width = master.shape
    pieces = owned // ROWS
    bf16, f32 = jnp.bfloat16, jnp.float32
    dma = pltpu.SemaphoreType.DMA
    shape = jax.ShapeDtypeStruct
    state = (1, owned, width)
    out_shapes = (
        (state, f32), (state, bf16), ((1, owned), f32),
        (state, bf16), ((1, owned), f32),
        ((1, 2 * outer * owned, width), bf16),
    )
    kept = sum(math.prod(dims) * jnp.dtype(kind).itemsize for dims, kind in out_shapes)
    outs = pl.pallas_call(
        functools.partial(kernel, outer),
        out_shape=tuple(pltpu.VMEM(*each) for each in out_shapes),
        in_specs=[pl.BlockSpec(memory_space=pltpu.HBM)] * 6,
        out_specs=[pl.BlockSpec(memory_space=pltpu.VMEM)] * 6,
        scratch_shapes=[
            pltpu.VMEM((pieces, outer, ROWS, width), bf16),
            pltpu.VMEM((pieces, outer, ROWS, width), bf16),
            pltpu.VMEM((pieces, outer, ROWS, width), bf16),
            pltpu.VMEM((pieces, ROWS, width), f32),
            pltpu.VMEM((pieces, outer, ROWS, width), bf16),
            pltpu.VMEM((pieces, outer // 2, ROWS, width), bf16),
            pltpu.VMEM(state, f32), pltpu.VMEM(state, bf16), pltpu.VMEM(state, bf16),
            pltpu.VMEM((1, owned), f32), pltpu.VMEM((1, owned), f32),
            dma((pieces, outer)), dma((5,)),
            dma((pieces, outer)), dma((pieces, outer)),
            dma((pieces, outer)), dma((pieces, outer)), dma((pieces, outer // 2)),
            dma((pieces, 2 * outer)), dma((pieces, 2 * outer)), dma((pieces, 2 * outer)),
            dma((pieces, outer)), dma((pieces, outer)),
        ],
        compiler_params=pltpu.CompilerParams(
            collective_id=0, has_side_effects=True,
            vmem_limit_bytes=min(VMEM_GRANT, VMEM_ALL - kept - 2**18),
        ),
    )(grads, master, m_codes, m_scale, v_codes, v_scale)
    return tuple(pl.pallas_call(
        write_out,
        out_shape=tuple(shape(*each) for each in out_shapes),
        in_specs=[pl.BlockSpec(memory_space=pltpu.VMEM)] * 6,
        out_specs=[pl.BlockSpec(memory_space=pl.ANY)] * 6,
        scratch_shapes=[dma((6,))],
        compiler_params=pltpu.CompilerParams(vmem_limit_bytes=2**20),
    )(*[pltpu.with_memory_space_constraint(o, pltpu.VMEM) for o in outs]))


def solution(mesh):
    return jax.shard_map(
        per_device,
        mesh=mesh,
        in_specs=(
            P("dp", "mp", None, None),
            P("mp", "dp", None),
            P("mp", "dp", None),
            P("mp", "dp"),
            P("mp", "dp", None),
            P("mp", "dp"),
        ),
        out_specs=(
            P("mp", "dp", None),
            P("mp", "dp", None),
            P("mp", "dp"),
            P("mp", "dp", None),
            P("mp", "dp"),
            P("mp", None, None),
        ),
        check_vma=False,
    )
```
